256 devices in a mesh: groups: 2 (over y), frame: 64 (over x, z), row: 2 (over core).
Axes of the slice: x: 4, y: 2, z: 16, core: 2. Of those that a mesh axis runs over, the one named last changes fastest.
The devices are a block of a 4x16x16 slice.
Arguments:
- latent: bfloat16 [128, 16, 64, 640], P(('groups', 'frame'), 'row'), parts along dimension 0, may hold values from -18 to 18
- norm_gain: float32 [640], replicated, may hold values from 0.1 to 1.9
- time_kernel: bfloat16 [3, 640, 640], replicated, may hold values from -0.125 to 0.125
- space_norm: float32 [640], replicated, may hold values from 0.1 to 1.9
- space_qkv: bfloat16 [640, 1920], replicated, may hold values from -12 to 12
- space_out: bfloat16 [640, 640], replicated, may hold values from -0.25 to 0.25
- time_norm: float32 [640], replicated, may hold values from 0.1 to 1.9
- time_qkv: bfloat16 [640, 1920], replicated, may hold values from -12 to 12
- time_out: bfloat16 [640, 640], replicated, may hold values from -0.25 to 0.25
Outputs:
- output: float32 [128, 16, 64, 640], P(('groups', 'frame'), 'row'), parts along dimension 0
The draws below stay inside these ranges and needn't reach their ends.
There are 2 independent parts, one for each index of `groups`. The reference program is written for one: setup_inputs(seed, part) draws one part's arguments, and reference() takes and returns one part's arrays. A program takes and returns all parts, laid end to end along the dimension named above; an argument that names none is the same for every part. Nothing has to cross between parts.
All inputs are finite; a program needn't handle non-finite values.
Results may differ from the reference program's by a relative error of at most 0.0018.
Values may be sent and summed in bfloat16 or wider, within the bound.
No kernel may reach another device: no remote copies, remote signals or barrier semaphores. Data moves between devices by JAX's collectives and lax.ppermute only.
A program may use at most 128 MiB of HBM per device.

```python
import jax
import jax.numpy as jnp
from jax import lax

C = 640
HEADS = 10
GROUPS = 32
WID = 64
FRAMES = 64
ROWS = 16


def projection_draw(key, salt):
    folded = jax.random.fold_in(key, salt)
    matrix = jax.random.normal(folded, (C, 3 * C), jnp.float32) / jnp.sqrt(jnp.float32(C))
    return jnp.clip(matrix, -12.0, 12.0).astype(jnp.bfloat16)


def draw_space_qkv(key, part):
    return projection_draw(key, 11)


def draw_time_qkv(key, part):
    return projection_draw(key, 23)


def draw_latent(key, part):
    folded = jax.random.fold_in(key, 37)
    offset_key = jax.random.fold_in(key, 41)
    sign_key = jax.random.fold_in(key, 43)
    position = jnp.arange(FRAMES, dtype=jnp.float32) / jnp.float32(max(FRAMES - 1, 1))
    magnitude = jax.random.uniform(offset_key, (GROUPS,), jnp.float32, 1.0, 2.5)
    signs = jnp.where(jax.random.uniform(sign_key, (GROUPS,), jnp.float32) < 0.5, -1.0, 1.0)
    group_offset = jnp.repeat(magnitude * signs, C // GROUPS)
    drift = (1.0 + 2.0 * position)[:, None, None, None] * group_offset[None, None, None, :]
    ramp = 1.0 + 2.0 * position
    values = jnp.clip(jax.random.normal(folded, (FRAMES, ROWS, WID, C), jnp.float32), -6.0, 6.0)
    return jnp.clip(values * ramp[:, None, None, None] + drift, -18.0, 18.0).astype(jnp.bfloat16)


def bell_draw(stream_key, dims, deviation, reach, kind=jnp.bfloat16):
    drawn = deviation * jax.random.normal(stream_key, dims, jnp.float32)
    return jnp.clip(drawn, min=-reach, max=reach).astype(kind)


def setup_inputs(seed: int = 0, part: int = 0) -> dict:
    key_list = jax.random.split(jax.random.key(seed), 10)
    part_splits = jax.random.split(jax.random.fold_in(key_list[9], part), 10)
    return {
        "latent": draw_latent(jax.random.fold_in(jax.random.fold_in(key_list[9], part), 71), part),
        "norm_gain": jnp.clip(1.0 + 0.18 * jax.random.normal(key_list[1], (C,), jnp.float32), 0.1, 1.9),
        "time_kernel": bell_draw(key_list[2], (3, C, C), (3 * C) ** -0.5, 0.125),
        "space_norm": jnp.clip(1.0 + 0.18 * jax.random.normal(key_list[3], (C,), jnp.float32), 0.1, 1.9),
        "space_qkv": draw_space_qkv(jax.random.fold_in(key_list[9], 71), part),
        "space_out": bell_draw(key_list[5], (C, C), C ** -0.5, 0.25),
        "time_norm": jnp.clip(1.0 + 0.18 * jax.random.normal(key_list[6], (C,), jnp.float32), 0.1, 1.9),
        "time_qkv": draw_time_qkv(jax.random.fold_in(key_list[9], 71), part),
        "time_out": bell_draw(key_list[8], (C, C), C ** -0.5, 0.25),
    }


epsilon = 1e-05

def normalize_silu(grouped, first, second, number, gain, shape):
    center = first / number
    spread = second / number - center * center
    scaling = lax.rsqrt(spread + epsilon)
    normed = ((grouped - center[:, None]) * scaling[:, None]).reshape(shape) * gain
    return jax.nn.silu(normed).astype(jnp.bfloat16)

def layer_norm(inputs, gain):
    widened = inputs.astype(jnp.float32)
    center = lax.optimization_barrier(jnp.mean(widened, axis=-1, keepdims=True))
    shifted = widened - center
    spread = lax.optimization_barrier(jnp.mean(shifted * shifted, axis=-1, keepdims=True))
    return (shifted * lax.rsqrt(spread + epsilon) * gain).astype(jnp.bfloat16)

def reference(latent, norm_gain, time_kernel, space_norm, space_qkv, space_out, time_norm, time_qkv, time_out):
    frames, row_count, col_count, channels = latent.shape
    pixels = row_count * col_count
    per_group = channels // GROUPS
    head_size = channels // HEADS
    scale = head_size ** (-0.5)
    grouped = latent.astype(jnp.float32).reshape(frames, row_count, col_count, GROUPS, per_group)
    first = lax.optimization_barrier(jnp.sum(grouped, axis=(0, 1, 2, 4)))
    second = lax.optimization_barrier(jnp.sum(grouped * grouped, axis=(0, 1, 2, 4)))
    number = frames * pixels * per_group
    hidden = normalize_silu(grouped, first, second, number, norm_gain, latent.shape)
    padded = jnp.pad(hidden, ((1, 1), (0, 0), (0, 0), (0, 0)))
    mixed = jnp.zeros((frames * pixels, channels), jnp.float32)
    for tap in range(3):
        window = padded[tap:tap + frames].reshape(-1, channels)
        mixed = mixed + jnp.dot(window, time_kernel[tap], preferred_element_type=jnp.float32)
    stepped = latent.astype(jnp.float32).reshape(-1, channels) + mixed
    tokens = layer_norm(stepped, space_norm)
    packed = jnp.dot(tokens, space_qkv, preferred_element_type=jnp.float32).astype(jnp.bfloat16)
    packed = packed.reshape(frames, pixels, 3, HEADS, head_size)

    def one_frame(block):
        queries = block[:, 0].astype(jnp.float32)
        key_rows = block[:, 1].astype(jnp.float32)
        values = block[:, 2].astype(jnp.float32)
        scores = jnp.einsum('qhd,khd->hqk', queries, key_rows) * scale
        raised = jnp.exp(scores - lax.optimization_barrier(jnp.max(scores, axis=-1, keepdims=True)))
        weight_sum = lax.optimization_barrier(jnp.sum(raised, axis=-1))
        weights = raised.astype(jnp.bfloat16).astype(jnp.float32)
        result = jnp.einsum('hqk,khd->qhd', weights, values) / jnp.transpose(weight_sum)[:, :, None]
        return result.astype(jnp.bfloat16).reshape(pixels, channels)
    attended = lax.map(one_frame, packed)
    spaced = stepped + jnp.dot(attended.reshape(-1, channels), space_out, preferred_element_type=jnp.float32)
    normed = layer_norm(spaced, time_norm)
    packed_time = jnp.dot(normed, time_qkv, preferred_element_type=jnp.float32).astype(jnp.bfloat16)
    packed_time = packed_time.reshape(frames, pixels, 3, HEADS, head_size).astype(jnp.float32)
    queries = packed_time[:, :, 0]
    key_rows = packed_time[:, :, 1]
    values = packed_time[:, :, 2]
    scores = jnp.einsum('qphd,kphd->phqk', queries, key_rows) * scale
    raised = jnp.exp(scores - lax.optimization_barrier(jnp.max(scores, axis=-1, keepdims=True)))
    weight_sum = lax.optimization_barrier(jnp.sum(raised, axis=-1))
    weights = raised.astype(jnp.bfloat16).astype(jnp.float32)
    result = jnp.einsum('phqk,kphd->qphd', weights, values) / jnp.transpose(weight_sum, (2, 0, 1))[:, :, :, None]
    attended_time = result.astype(jnp.bfloat16).reshape(-1, channels)
    output = spaced + jnp.dot(attended_time, time_out, preferred_element_type=jnp.float32)
    return output.reshape(frames, row_count, col_count, channels)
```

```python
import functools

import jax
import jax.numpy as jnp
from jax import lax
from jax.experimental import pallas as pl
from jax.experimental.pallas import tpu as pltpu
from jax.sharding import PartitionSpec as P

HEADS = 10
GROUPS = 32
FRAME = "frame"
FRAME_ROW = ("frame", "row")
LOG2E = 1.4426950408889634

epsilon = 1e-05
f32 = jnp.float32
bf16 = jnp.bfloat16


def vmem():
    return pl.BlockSpec(memory_space=pltpu.VMEM)


def params(mib):
    return pltpu.CompilerParams(vmem_limit_bytes=mib << 20)


def cost(flops, nbytes, trans=0):
    return pl.CostEstimate(flops=flops, bytes_accessed=nbytes, transcendentals=trans)


def dot(a, b, dims=((1,), (0,)), precision=None):
    return lax.dot_general(
        a, b, (dims, ((), ())), preferred_element_type=f32, precision=precision
    )


def group_slots(channels, offset):
    per_group = channels // GROUPS
    slot = lax.broadcasted_iota(jnp.int32, (128, channels), 0)
    chan = lax.broadcasted_iota(jnp.int32, (128, channels), 1)
    low = (slot - offset) * per_group
    inside = (chan >= low) & (chan < low + per_group)
    return jnp.where(inside, 1.0, 0.0).astype(f32)


def layer_norm(inputs, gain):
    center = jnp.mean(inputs, axis=-1, keepdims=True)
    shifted = inputs - center
    spread = jnp.mean(shifted * shifted, axis=-1, keepdims=True)
    return (shifted * lax.rsqrt(spread + epsilon) * gain).astype(bf16)


def sums_kernel(x_ref, o_ref, acc):
    step = pl.program_id(0)
    x = x_ref[...].astype(f32)
    rows, channels = x.shape
    part = x.reshape(rows // 8, 8, channels)
    first, second = jnp.sum(part, axis=0), jnp.sum(part * part, axis=0)

    @pl.when(step == 0)
    def _():
        acc[0] = first
        acc[1] = second

    @pl.when(step > 0)
    def _():
        acc[0] += first
        acc[1] += second

    @pl.when(step == pl.num_programs(0) - 1)
    def _():
        exact = lax.Precision.HIGHEST
        total = dot(acc[0], group_slots(channels, 0), ((1,), (1,)), exact)
        total += dot(acc[1], group_slots(channels, GROUPS), ((1,), (1,)), exact)
        row = jnp.sum(total, axis=0, keepdims=True)
        o_ref[...] = jnp.broadcast_to(row[None], o_ref.shape)


def group_sums(latent, members):
    rows, channels = latent.shape
    tile = rows // 2
    return pl.pallas_call(
        sums_kernel,
        out_shape=jax.ShapeDtypeStruct((members, 1, 128), f32),
        grid=(rows // tile,),
        in_specs=[pl.BlockSpec((tile, channels), lambda i: (i, 0))],
        out_specs=pl.BlockSpec((members, 1, 128), lambda i: (0, 0, 0)),
        scratch_shapes=[pltpu.VMEM((2, 8, channels), f32)],
        compiler_params=params(16),
        cost_estimate=cost(4 * rows * channels, 2 * rows * channels),
        name="group_sums",
    )(latent)


def front_kernel(
    number, edge_ref, sums_ref, gain_ref, low_ref, mid_ref, high_ref, kernel_ref, norm_ref,
    stepped_ref, tokens_ref, scale
):
    channels = mid_ref.shape[1]

    @pl.when(pl.program_id(0) == 0)
    def _():
        exact = lax.Precision.HIGHEST
        total = jnp.broadcast_to(jnp.sum(sums_ref[...], axis=0), (8, 128))
        center = dot(total, group_slots(channels, 0), precision=exact) / number
        square = dot(total, group_slots(channels, GROUPS), precision=exact) / number
        scaling = lax.rsqrt(square - center * center + epsilon) * gain_ref[...]
        scale[0] = scaling
        scale[1] = center

    scaling, center = scale[0, 0:1], scale[1, 0:1]

    def hidden(ref):
        half = 0.5 * ((ref[...].astype(f32) - center) * scaling)
        return (half + half * jnp.tanh(half)).astype(bf16)

    low = hidden(low_ref)
    low = jnp.where(edge_ref[0] > 0, low, jnp.zeros_like(low))
    high = hidden(high_ref)
    high = jnp.where(edge_ref[1] > 0, high, jnp.zeros_like(high))
    mixed = dot(low, kernel_ref[0])
    mixed += dot(hidden(mid_ref), kernel_ref[1])
    mixed += dot(high, kernel_ref[2])
    stepped = mid_ref[...].astype(f32) + mixed
    stepped_ref[...] = stepped
    tokens_ref[...] = layer_norm(stepped, norm_ref[...])


def front(edge, sums, gain, low, mid, high, time_kernel, norm, number):
    rows, channels = mid.shape
    tile = rows // 2
    block = pl.BlockSpec((tile, channels), lambda i: (i, 0))
    one = pl.BlockSpec((1, channels), lambda i: (0, 0))
    return pl.pallas_call(
        functools.partial(front_kernel, number),
        out_shape=[
            jax.ShapeDtypeStruct((rows, channels), f32),
            jax.ShapeDtypeStruct((rows, channels), bf16),
        ],
        grid=(rows // tile,),
        in_specs=[
            pl.BlockSpec(memory_space=pltpu.SMEM),
            vmem(),
            one,
            block,
            block,
            block,
            vmem(),
            one,
        ],
        out_specs=[block, block],
        scratch_shapes=[pltpu.VMEM((2, 8, channels), f32)],
        compiler_params=params(24),
        cost_estimate=cost(6 * rows * channels * channels, 14 * rows * channels),
        name="front",
    )(edge, sums, gain, low, mid, high, time_kernel, norm)


def half_masks(shape):
    lane = lax.broadcasted_iota(jnp.int32, shape, len(shape) - 1)
    even = jnp.where(lane < 64, 1.0, 0.0).astype(bf16)
    odd = jnp.where(lane < 64, 0.0, 1.0).astype(bf16)
    return even, odd


def space_kernel(
    own_ref, peer_ref, stepped_ref, qkv_ref, out_ref, norm_ref, spaced_ref, normed_ref,
    queries, keys, values, attended
):
    rows, channels = own_ref.shape
    pairs = channels // 128
    length = 2 * rows
    even, odd = half_masks((rows, 128))
    for half, ref in enumerate((own_ref, peer_ref)):
        packed = dot(ref[...], qkv_ref[:, channels:]).astype(bf16)
        at = half * rows
        for j in range(pairs):
            k = packed[:, j * 128 : j * 128 + 128]
            v = packed[:, channels + j * 128 : channels + j * 128 + 128]
            for part, mask in enumerate((even, odd)):
                low = part * length + at
                keys[j, low : low + rows] = k * mask
                values[j, low : low + rows, :128] = v * mask
                values[j, low : low + rows, 128:] = mask
    packed = dot(own_ref[...], qkv_ref[:, :channels]).astype(bf16)
    for j in range(pairs):
        queries[j] = packed[:, j * 128 : j * 128 + 128]

    factor = 64 ** (-0.5) * LOG2E

    def pair(j, carry):
        q = queries[j]
        total = None
        for part in range(2):
            low = part * length
            scores = dot(q, keys[j, low : low + length], ((1,), (1,)))
            top = jnp.max(scores, axis=-1, keepdims=True)
            weights = jnp.exp2((scores - top) * factor).astype(bf16)
            found = dot(weights, values[j, low : low + length])
            total = found if total is None else total + found
        attended[j] = (total[:, :128] / total[:, 128:]).astype(bf16)
        return carry

    lax.fori_loop(0, pairs, pair, 0)
    joined = jnp.concatenate([attended[j] for j in range(pairs)], axis=1)
    spaced = stepped_ref[...] + dot(joined, out_ref[...])
    spaced_ref[...] = spaced
    normed_ref[...] = layer_norm(spaced, norm_ref[...])


def space(own, peer, stepped, qkv, out, norm):
    rows, channels = own.shape
    pairs = channels // 128
    return pl.pallas_call(
        space_kernel,
        out_shape=[
            jax.ShapeDtypeStruct((rows, channels), f32),
            jax.ShapeDtypeStruct((rows, channels), bf16),
        ],
        in_specs=[vmem()] * 6,
        out_specs=[vmem()] * 2,
        scratch_shapes=[
            pltpu.VMEM((pairs, rows, 128), bf16),
            pltpu.VMEM((pairs, 4 * rows, 128), bf16),
            pltpu.VMEM((pairs, 4 * rows, 256), bf16),
            pltpu.VMEM((pairs, rows, 128), bf16),
        ],
        compiler_params=params(40),
        cost_estimate=cost(12 * rows * channels * channels + 8 * rows * rows * channels, 14 * rows * channels, 2 * HEADS * rows * rows),
        name="space",
    )(own, peer, stepped, qkv, out, norm)


def time_kernel_body(x_ref, qkv_ref, o_ref, packed_ref, attended):
    frames, pixels, channels = x_ref.shape
    rows = frames * pixels
    pairs = channels // 128
    i = lax.broadcasted_iota(jnp.int32, (rows, rows), 0)
    j = lax.broadcasted_iota(jnp.int32, (rows, rows), 1)
    order = (j == (i % frames) * pixels + i // frames).astype(f32).astype(bf16)
    sorted_rows = dot(order, x_ref[...].reshape(rows, channels)).astype(bf16)
    packed_ref[...] = dot(sorted_rows, qkv_ref[...]).astype(bf16)
    factor = 64 ** (-0.5) * LOG2E
    even, odd = half_masks((frames, 128))
    left = lax.broadcasted_iota(jnp.int32, (frames, 128), 1) < 64
    low = jnp.full((frames, 128), -jnp.inf, f32)

    def pixel(p, carry):
        at = pl.multiple_of(p * frames, frames)
        for j in range(pairs):
            q = packed_ref[pl.ds(at, frames), j * 128 : j * 128 + 128]
            k = packed_ref[pl.ds(at, frames), channels + j * 128 : channels + j * 128 + 128]
            v = packed_ref[
                pl.ds(at, frames), 2 * channels + j * 128 : 2 * channels + j * 128 + 128
            ]
            scores = dot(q, jnp.concatenate([k * even, k * odd], axis=0), ((1,), (1,)))
            top_even = jnp.max(jnp.where(left, scores, low), axis=-1, keepdims=True)
            top_odd = jnp.max(jnp.where(left, low, scores), axis=-1, keepdims=True)
            top = jnp.where(left, top_even, top_odd)
            weights = jnp.exp2((scores - top) * factor).astype(bf16)
            both = jnp.concatenate(
                [
                    jnp.concatenate([v * even, even], axis=1),
                    jnp.concatenate([v * odd, odd], axis=1),
                ],
                axis=0,
            )
            found = dot(weights, both)
            attended[pl.ds(at, frames), j * 128 : j * 128 + 128] = (
                found[:, :128] / found[:, 128:]
            ).astype(bf16)
        return carry

    lax.fori_loop(0, pixels, pixel, 0)
    back = dot(order, attended[...], ((0,), (0,))).astype(bf16)
    o_ref[...] = back.reshape(frames, pixels, channels)


def time_attend(x, qkv):
    frames, pixels, channels = x.shape
    rows = frames * pixels
    return pl.pallas_call(
        time_kernel_body,
        out_shape=jax.ShapeDtypeStruct(x.shape, bf16),
        in_specs=[vmem()] * 2,
        out_specs=vmem(),
        scratch_shapes=[
            pltpu.VMEM((rows, 3 * channels), bf16),
            pltpu.VMEM((rows, channels), bf16),
        ],
        compiler_params=params(32),
        cost_estimate=cost(6 * rows * channels * channels + 4 * rows * rows * channels, 4 * rows * channels, HEADS * rows * frames),
        name="time_attend",
    )(x, qkv)


def finish_kernel(base_ref, x_ref, w_ref, o_ref):
    o_ref[...] = base_ref[...] + dot(x_ref[...], w_ref[...])


def finish(base, x, w):
    rows, channels = base.shape
    tile = rows // 4
    block = pl.BlockSpec((tile, channels), lambda i: (i, 0))
    return pl.pallas_call(
        finish_kernel,
        out_shape=jax.ShapeDtypeStruct((rows, channels), f32),
        grid=(rows // tile,),
        in_specs=[block, block, vmem()],
        out_specs=block,
        compiler_params=params(16),
        cost_estimate=cost(2 * rows * channels * channels, 10 * rows * channels),
        name="finish",
    )(base, x, w)


def body(
    latent, norm_gain, time_kernel, space_norm, space_qkv, space_out, time_norm, time_qkv, time_out
):
    frames, row_count, col_count, channels = latent.shape
    pixels = row_count * col_count
    assert frames == 1
    mine = latent.reshape(pixels, channels)
    count = lax.axis_size(FRAME)
    forward = [(i, i + 1) for i in range(count - 1)]
    backward = [(target, source) for source, target in forward]
    low = lax.ppermute(mine, FRAME, forward)
    high = lax.ppermute(mine, FRAME, backward)
    members = lax.axis_size(FRAME_ROW)
    sums = group_sums(mine, members)
    sums = lax.all_to_all(sums, FRAME_ROW, split_axis=0, concat_axis=0, tiled=True)
    number = float(members * pixels * (channels // GROUPS))
    here = lax.axis_index(FRAME)
    edge = jnp.stack([here > 0, here < count - 1]).astype(jnp.int32)
    stepped, tokens = front(
        edge, sums, norm_gain.reshape(1, -1), low, mine, high, time_kernel,
        space_norm.reshape(1, -1), number,
    )
    peer = lax.ppermute(tokens, "row", [(0, 1), (1, 0)])
    spaced, normed = space(tokens, peer, stepped, space_qkv, space_out, time_norm.reshape(1, -1))
    moved = lax.all_to_all(
        normed.reshape(count, pixels // count, channels),
        FRAME, split_axis=0, concat_axis=0, tiled=True,
    )
    result = time_attend(moved, time_qkv)
    back = lax.all_to_all(result, FRAME, split_axis=0, concat_axis=0, tiled=True)
    output = finish(spaced, back.reshape(pixels, channels), time_out)
    return output.reshape(frames, row_count, col_count, channels)


def solution(mesh):
    split = P(("groups", "frame"), "row", None, None)
    return jax.shard_map(
        body,
        mesh=mesh,
        in_specs=(split,) + (P(),) * 8,
        out_specs=split,
        check_vma=False,
    )
```

```python
import functools

import jax
import jax.numpy as jnp
from jax import lax
from jax.experimental import pallas as pl
from jax.experimental.pallas import tpu as pltpu
from jax.sharding import PartitionSpec as P

HEADS = 10
GROUPS = 32
FRAME = "frame"
FRAME_ROW = ("frame", "row")
LOG2E = 1.4426950408889634

epsilon = 1e-05
f32 = jnp.float32
bf16 = jnp.bfloat16


def vmem():
    return pl.BlockSpec(memory_space=pltpu.VMEM)


def params(mib):
    return pltpu.CompilerParams(vmem_limit_bytes=mib << 20)


def cost(flops, nbytes, trans=0):
    return pl.CostEstimate(flops=flops, bytes_accessed=nbytes, transcendentals=trans)


def dot(a, b, dims=((1,), (0,)), precision=None):
    return lax.dot_general(
        a, b, (dims, ((), ())), preferred_element_type=f32, precision=precision
    )


def group_slots(channels, offset):
    per_group = channels // GROUPS
    slot = lax.broadcasted_iota(jnp.int32, (128, channels), 0)
    chan = lax.broadcasted_iota(jnp.int32, (128, channels), 1)
    low = (slot - offset) * per_group
    inside = (chan >= low) & (chan < low + per_group)
    return jnp.where(inside, 1.0, 0.0).astype(f32)


def layer_norm(inputs, gain):
    center = jnp.mean(inputs, axis=-1, keepdims=True)
    shifted = inputs - center
    spread = jnp.mean(shifted * shifted, axis=-1, keepdims=True)
    return (shifted * lax.rsqrt(spread + epsilon) * gain).astype(bf16)


def sums_kernel(x_ref, o_ref, acc):
    step = pl.program_id(0)
    x = x_ref[...].astype(f32)
    rows, channels = x.shape
    part = x.reshape(rows // 8, 8, channels)
    first, second = jnp.sum(part, axis=0), jnp.sum(part * part, axis=0)

    @pl.when(step == 0)
    def _():
        acc[0] = first
        acc[1] = second

    @pl.when(step > 0)
    def _():
        acc[0] += first
        acc[1] += second

    @pl.when(step == pl.num_programs(0) - 1)
    def _():
        exact = lax.Precision.HIGHEST
        total = dot(acc[0], group_slots(channels, 0), ((1,), (1,)), exact)
        total += dot(acc[1], group_slots(channels, GROUPS), ((1,), (1,)), exact)
        row = jnp.sum(total, axis=0, keepdims=True)
        o_ref[...] = jnp.broadcast_to(row[None], o_ref.shape)


def group_sums(latent, members):
    rows, channels = latent.shape
    tile = rows // 2
    return pl.pallas_call(
        sums_kernel,
        out_shape=jax.ShapeDtypeStruct((members, 1, 128), f32),
        grid=(rows // tile,),
        in_specs=[pl.BlockSpec((tile, channels), lambda i: (i, 0))],
        out_specs=pl.BlockSpec((members, 1, 128), lambda i: (0, 0, 0)),
        scratch_shapes=[pltpu.VMEM((2, 8, channels), f32)],
        compiler_params=params(16),
        cost_estimate=cost(4 * rows * channels, 2 * rows * channels),
        name="group_sums",
    )(latent)


def front_kernel(
    number, edge_ref, sums_ref, gain_ref, low_ref, mid_ref, high_ref, kernel_ref, norm_ref,
    stepped_ref, tokens_ref, scale
):
    channels = mid_ref.shape[1]

    @pl.when(pl.program_id(0) == 0)
    def _():
        exact = lax.Precision.HIGHEST
        total = jnp.broadcast_to(jnp.sum(sums_ref[...], axis=0), (8, 128))
        center = dot(total, group_slots(channels, 0), precision=exact) / number
        square = dot(total, group_slots(channels, GROUPS), precision=exact) / number
        scaling = lax.rsqrt(square - center * center + epsilon) * gain_ref[...]
        scale[0] = scaling
        scale[1] = center

    scaling, center = scale[0, 0:1], scale[1, 0:1]

    def hidden(ref):
        half = 0.5 * ((ref[...].astype(f32) - center) * scaling)
        return (half + half * jnp.tanh(half)).astype(bf16)

    low = hidden(low_ref)
    low = jnp.where(edge_ref[0] > 0, low, jnp.zeros_like(low))
    high = hidden(high_ref)
    high = jnp.where(edge_ref[1] > 0, high, jnp.zeros_like(high))
    mixed = dot(low, kernel_ref[0])
    mixed += dot(hidden(mid_ref), kernel_ref[1])
    mixed += dot(high, kernel_ref[2])
    stepped = mid_ref[...].astype(f32) + mixed
    stepped_ref[...] = stepped
    tokens_ref[...] = layer_norm(stepped, norm_ref[...])


def front(edge, sums, gain, low, mid, high, time_kernel, norm, number):
    rows, channels = mid.shape
    tile = rows // 2
    block = pl.BlockSpec((tile, channels), lambda i: (i, 0))
    one = pl.BlockSpec((1, channels), lambda i: (0, 0))
    return pl.pallas_call(
        functools.partial(front_kernel, number),
        out_shape=[
            jax.ShapeDtypeStruct((rows, channels), f32),
            jax.ShapeDtypeStruct((rows, channels), bf16),
        ],
        grid=(rows // tile,),
        in_specs=[
            pl.BlockSpec(memory_space=pltpu.SMEM),
            vmem(),
            one,
            block,
            block,
            block,
            vmem(),
            one,
        ],
        out_specs=[block, block],
        scratch_shapes=[pltpu.VMEM((2, 8, channels), f32)],
        compiler_params=params(24),
        cost_estimate=cost(6 * rows * channels * channels, 14 * rows * channels),
        name="front",
    )(edge, sums, gain, low, mid, high, time_kernel, norm)


def half_masks(shape):
    lane = lax.broadcasted_iota(jnp.int32, shape, len(shape) - 1)
    even = jnp.where(lane < 64, 1.0, 0.0).astype(bf16)
    odd = jnp.where(lane < 64, 0.0, 1.0).astype(bf16)
    return even, odd


def space_kernel(
    own_ref, peer_ref, stepped_ref, qkv_ref, out_ref, norm_ref, spaced_ref, normed_ref,
    queries, keys, values, attended
):
    rows, channels = own_ref.shape
    pairs = channels // 128
    length = 2 * rows
    even, odd = half_masks((rows, 128))
    for half, ref in enumerate((own_ref, peer_ref)):
        packed = dot(ref[...], qkv_ref[:, channels:]).astype(bf16)
        at = half * rows
        for j in range(pairs):
            k = packed[:, j * 128 : j * 128 + 128]
            keys[j, at : at + rows] = k * even
            keys[j, length + at : length + at + rows] = k * odd
            v = packed[:, channels + j * 128 : channels + j * 128 + 128].T
            values[j, :128, at : at + rows] = v
            values[j, 128:, at : at + rows] = jnp.ones((16, rows), bf16)
    packed = dot(own_ref[...], qkv_ref[:, :channels]).astype(bf16)
    for j in range(pairs):
        queries[j] = packed[:, j * 128 : j * 128 + 128].T

    factor = 64 ** (-0.5) * LOG2E

    def pair(j, carry):
        q = queries[j]
        weights = []
        for part in range(2):
            low = part * length
            scores = dot(keys[j, low : low + length], q)
            top = jnp.max(scores, axis=0, keepdims=True)
            weights.append(jnp.exp2((scores - top) * factor).astype(bf16))
        first = dot(values[j], weights[0])
        second = dot(values[j], weights[1])
        first = first[:64] / first[128:129]
        second = second[64:128] / second[128:129]
        attended[j] = jnp.concatenate([first, second], axis=0).T.astype(bf16)
        return carry

    lax.fori_loop(0, pairs, pair, 0, unroll=True)
    joined = jnp.concatenate([attended[j] for j in range(pairs)], axis=1)
    spaced = stepped_ref[...] + dot(joined, out_ref[...])
    spaced_ref[...] = spaced
    normed_ref[...] = layer_norm(spaced, norm_ref[...])


def space(own, peer, stepped, qkv, out, norm):
    rows, channels = own.shape
    pairs = channels // 128
    return pl.pallas_call(
        space_kernel,
        out_shape=[
            jax.ShapeDtypeStruct((rows, channels), f32),
            jax.ShapeDtypeStruct((rows, channels), bf16),
        ],
        in_specs=[vmem()] * 6,
        out_specs=[vmem()] * 2,
        scratch_shapes=[
            pltpu.VMEM((pairs, 128, rows), bf16),
            pltpu.VMEM((pairs, 4 * rows, 128), bf16),
            pltpu.VMEM((pairs, 144, 2 * rows), bf16),
            pltpu.VMEM((pairs, rows, 128), bf16),
        ],
        compiler_params=params(40),
        cost_estimate=cost(12 * rows * channels * channels + 8 * rows * rows * channels, 14 * rows * channels, 2 * HEADS * rows * rows),
        name="space",
    )(own, peer, stepped, qkv, out, norm)


def time_kernel_body(x_ref, qkv_ref, o_ref, packed_ref, turned, attended):
    frames, pixels, channels = x_ref.shape
    rows = frames * pixels
    pairs = channels // 128
    i = lax.broadcasted_iota(jnp.int32, (rows, rows), 0)
    j = lax.broadcasted_iota(jnp.int32, (rows, rows), 1)
    order = (j == (i % frames) * pixels + i // frames).astype(f32).astype(bf16)
    sorted_rows = dot(order, x_ref[...].reshape(rows, channels)).astype(bf16)
    packed = dot(sorted_rows, qkv_ref[...]).astype(bf16)
    packed_ref[...] = packed
    turned[...] = packed[:, channels : 2 * channels].T
    factor = 64 ** (-0.5) * LOG2E
    even, odd = half_masks((128, 128))
    above = lax.broadcasted_iota(jnp.int32, (128, 128), 0) < 64
    left = lax.broadcasted_iota(jnp.int32, (128, 128), 1) < 64
    same = above == left
    zero = jnp.zeros((128, 128), bf16)

    def two_pixels(at):
        for j in range(pairs):
            lanes = slice(j * 128, j * 128 + 128)
            q = packed_ref[at, lanes]
            v = packed_ref[at, 2 * channels + j * 128 : 2 * channels + j * 128 + 128]
            k = turned[lanes, at]
            keys = jnp.concatenate([jnp.where(above, k, zero), jnp.where(above, zero, k)], axis=1)
            scores = dot(q, keys)
            parts = []
            for part in range(2):
                own = jnp.where(same, scores[:, part * 128 : part * 128 + 128], -jnp.inf)
                top = jnp.max(own, axis=-1, keepdims=True)
                parts.append(jnp.exp2((own - top) * factor).astype(bf16))
            both = jnp.concatenate(
                [
                    jnp.concatenate([v * even, even], axis=1),
                    jnp.concatenate([v * odd, odd], axis=1),
                ],
                axis=0,
            )
            found = dot(jnp.concatenate(parts, axis=1), both)
            attended[at, lanes] = (found[:, :128] / found[:, 128:]).astype(bf16)

    for p in range(pixels // 2):
        two_pixels(slice(p * 128, p * 128 + 128))
    back = dot(order, attended[...], ((0,), (0,))).astype(bf16)
    o_ref[...] = back.reshape(frames, pixels, channels)


def time_attend(x, qkv):
    frames, pixels, channels = x.shape
    rows = frames * pixels
    return pl.pallas_call(
        time_kernel_body,
        out_shape=jax.ShapeDtypeStruct(x.shape, bf16),
        in_specs=[vmem()] * 2,
        out_specs=vmem(),
        scratch_shapes=[
            pltpu.VMEM((rows, 3 * channels), bf16),
            pltpu.VMEM((channels, rows), bf16),
            pltpu.VMEM((rows, channels), bf16),
        ],
        compiler_params=params(32),
        cost_estimate=cost(6 * rows * channels * channels + 4 * rows * rows * channels, 4 * rows * channels, HEADS * rows * frames),
        name="time_attend",
    )(x, qkv)


def finish_kernel(base_ref, x_ref, w_ref, o_ref):
    o_ref[...] = base_ref[...] + dot(x_ref[...], w_ref[...])


def finish(base, x, w):
    rows, channels = base.shape
    tile = rows // 4
    block = pl.BlockSpec((tile, channels), lambda i: (i, 0))
    return pl.pallas_call(
        finish_kernel,
        out_shape=jax.ShapeDtypeStruct((rows, channels), f32),
        grid=(rows // tile,),
        in_specs=[block, block, vmem()],
        out_specs=block,
        compiler_params=params(16),
        cost_estimate=cost(2 * rows * channels * channels, 10 * rows * channels),
        name="finish",
    )(base, x, w)


def body(
    latent, norm_gain, time_kernel, space_norm, space_qkv, space_out, time_norm, time_qkv, time_out
):
    frames, row_count, col_count, channels = latent.shape
    pixels = row_count * col_count
    assert frames == 1
    mine = latent.reshape(pixels, channels)
    count = lax.axis_size(FRAME)
    forward = [(i, i + 1) for i in range(count - 1)]
    backward = [(target, source) for source, target in forward]
    low = lax.ppermute(mine, FRAME, forward)
    high = lax.ppermute(mine, FRAME, backward)
    members = lax.axis_size(FRAME_ROW)
    sums = group_sums(mine, members)
    sums = lax.all_to_all(sums, FRAME_ROW, split_axis=0, concat_axis=0, tiled=True)
    number = float(members * pixels * (channels // GROUPS))
    here = lax.axis_index(FRAME)
    edge = jnp.stack([here > 0, here < count - 1]).astype(jnp.int32)
    stepped, tokens = front(
        edge, sums, norm_gain.reshape(1, -1), low, mine, high, time_kernel,
        space_norm.reshape(1, -1), number,
    )
    peer = lax.ppermute(tokens, "row", [(0, 1), (1, 0)])
    spaced, normed = space(tokens, peer, stepped, space_qkv, space_out, time_norm.reshape(1, -1))
    moved = lax.all_to_all(
        normed.reshape(count, pixels // count, channels),
        FRAME, split_axis=0, concat_axis=0, tiled=True,
    )
    result = time_attend(moved, time_qkv)
    back = lax.all_to_all(result, FRAME, split_axis=0, concat_axis=0, tiled=True)
    output = finish(spaced, back.reshape(pixels, channels), time_out)
    return output.reshape(frames, row_count, col_count, channels)


def solution(mesh):
    split = P(("groups", "frame"), "row", None, None)
    return jax.shard_map(
        body,
        mesh=mesh,
        in_specs=(split,) + (P(),) * 8,
        out_specs=split,
        check_vma=False,
    )
```

```python
import functools

import jax
import jax.numpy as jnp
from jax import lax
from jax.experimental import pallas as pl
from jax.experimental.pallas import tpu as pltpu
from jax.sharding import PartitionSpec as P

HEADS = 10
GROUPS = 32
FRAME = "frame"
FRAME_ROW = ("frame", "row")
LOG2E = 1.4426950408889634

epsilon = 1e-05
f32 = jnp.float32
bf16 = jnp.bfloat16


def vmem():
    return pl.BlockSpec(memory_space=pltpu.VMEM)


def params(mib):
    return pltpu.CompilerParams(vmem_limit_bytes=mib << 20)


def cost(flops, nbytes, trans=0):
    return pl.CostEstimate(flops=flops, bytes_accessed=nbytes, transcendentals=trans)


def dot(a, b, dims=((1,), (0,)), precision=None):
    return lax.dot_general(
        a, b, (dims, ((), ())), preferred_element_type=f32, precision=precision
    )


def group_slots(channels, offset):
    per_group = channels // GROUPS
    slot = lax.broadcasted_iota(jnp.int32, (128, channels), 0)
    chan = lax.broadcasted_iota(jnp.int32, (128, channels), 1)
    low = (slot - offset) * per_group
    inside = (chan >= low) & (chan < low + per_group)
    return jnp.where(inside, 1.0, 0.0).astype(f32)


def layer_norm(inputs, gain):
    center = jnp.mean(inputs, axis=-1, keepdims=True)
    shifted = inputs - center
    spread = jnp.mean(shifted * shifted, axis=-1, keepdims=True)
    return (shifted * lax.rsqrt(spread + epsilon) * gain).astype(bf16)


def sums_kernel(x_ref, o_ref, near, sem):
    rows, channels = x_ref.shape
    parts = 4
    tile = rows // parts
    copies = [
        pltpu.make_async_copy(
            x_ref.at[i * tile : i * tile + tile], near.at[i * tile : i * tile + tile], sem.at[i]
        )
        for i in range(parts)
    ]
    for copy in copies:
        copy.start()
    first = jnp.zeros((8, channels), f32)
    second = jnp.zeros((8, channels), f32)
    slots, later = group_slots(channels, 0), group_slots(channels, GROUPS)
    for i, copy in enumerate(copies):
        copy.wait()
        x = near[i * tile : i * tile + tile].astype(f32).reshape(tile // 8, 8, channels)
        first += jnp.sum(x, axis=0)
        second += jnp.sum(x * x, axis=0)
    exact = lax.Precision.HIGHEST
    total = dot(first, slots, ((1,), (1,)), exact) + dot(second, later, ((1,), (1,)), exact)
    row = jnp.sum(total, axis=0, keepdims=True)
    o_ref[...] = jnp.broadcast_to(row[None], o_ref.shape)


def group_sums(latent, members):
    rows, channels = latent.shape
    return pl.pallas_call(
        sums_kernel,
        out_shape=jax.ShapeDtypeStruct((members, 1, 128), f32),
        in_specs=[pl.BlockSpec(memory_space=pltpu.HBM)],
        out_specs=vmem(),
        scratch_shapes=[pltpu.VMEM((rows, channels), bf16), pltpu.SemaphoreType.DMA((4,))],
        compiler_params=params(16),
        cost_estimate=cost(4 * rows * channels, 2 * rows * channels),
        name="group_sums",
    )(pin(latent))


def pin(x):
    return pltpu.with_memory_space_constraint(x, pltpu.HBM)


def front_kernel(
    number, edge_ref, sums_ref, gain_ref, low_ref, mid_ref, high_ref, kernel_far, norm_ref,
    stepped_ref, tokens_ref, scale, kernel_ref, sem
):
    channels = mid_ref.shape[1]
    first_step = pl.program_id(0) == 0
    get_kernel = pltpu.make_async_copy(kernel_far, kernel_ref, sem)

    @pl.when(first_step)
    def _():
        get_kernel.start()
        exact = lax.Precision.HIGHEST
        total = jnp.broadcast_to(jnp.sum(sums_ref[...], axis=0), (8, 128))
        center = dot(total, group_slots(channels, 0), precision=exact) / number
        square = dot(total, group_slots(channels, GROUPS), precision=exact) / number
        scaling = lax.rsqrt(square - center * center + epsilon) * gain_ref[...]
        scale[0] = scaling
        scale[1] = center
        get_kernel.wait()

    scaling, center = scale[0, 0:1], scale[1, 0:1]

    def hidden(ref):
        half = 0.5 * ((ref[...].astype(f32) - center) * scaling)
        return (half + half * jnp.tanh(half)).astype(bf16)

    low = hidden(low_ref)
    low = jnp.where(edge_ref[0] > 0, low, jnp.zeros_like(low))
    high = hidden(high_ref)
    high = jnp.where(edge_ref[1] > 0, high, jnp.zeros_like(high))
    mixed = dot(low, kernel_ref[0])
    mixed += dot(hidden(mid_ref), kernel_ref[1])
    mixed += dot(high, kernel_ref[2])
    stepped = mid_ref[...].astype(f32) + mixed
    stepped_ref[...] = stepped
    tokens_ref[...] = layer_norm(stepped, norm_ref[...])


def front(edge, sums, gain, low, mid, high, time_kernel, norm, number):
    rows, channels = mid.shape
    tile = rows // 2
    block = pl.BlockSpec((tile, channels), lambda i: (i, 0))
    one = pl.BlockSpec((1, channels), lambda i: (0, 0))
    return pl.pallas_call(
        functools.partial(front_kernel, number),
        out_shape=[
            jax.ShapeDtypeStruct((rows, channels), f32),
            jax.ShapeDtypeStruct((rows, channels), bf16),
        ],
        grid=(rows // tile,),
        in_specs=[
            pl.BlockSpec(memory_space=pltpu.SMEM),
            vmem(),
            one,
            block,
            block,
            block,
            pl.BlockSpec(memory_space=pltpu.HBM),
            one,
        ],
        out_specs=[block, block],
        scratch_shapes=[
            pltpu.VMEM((2, 8, channels), f32),
            pltpu.VMEM(time_kernel.shape, bf16),
            pltpu.SemaphoreType.DMA,
        ],
        compiler_params=params(24),
        cost_estimate=cost(6 * rows * channels * channels, 14 * rows * channels),
        name="front",
    )(edge, sums, gain, low, pin(mid), high, pin(time_kernel), norm)


def half_masks(shape):
    lane = lax.broadcasted_iota(jnp.int32, shape, len(shape) - 1)
    even = jnp.where(lane < 64, 1.0, 0.0).astype(bf16)
    odd = jnp.where(lane < 64, 0.0, 1.0).astype(bf16)
    return even, odd


def split_heads(packed, keys, values, at=0):
    rows, width = packed.shape
    channels = width // 2
    even, odd = half_masks((rows, 128))
    for j in range(channels // 128):
        k = packed[:, j * 128 : j * 128 + 128]
        v = packed[:, channels + j * 128 : channels + j * 128 + 128].T
        keys[j, 0, at : at + rows] = k * even
        keys[j, 1, at : at + rows] = k * odd
        values[j, :128, at : at + rows] = v
        values[j, 128:, at : at + rows] = jnp.ones((16, rows), bf16)


def project_kernel(own_ref, qkv_ref, queries, keys, values):
    channels = own_ref.shape[1]
    own = own_ref[...]
    packed = dot(own, qkv_ref[:, :channels]).astype(bf16)
    for j in range(channels // 128):
        queries[j] = packed[:, j * 128 : j * 128 + 128].T
    split_heads(dot(own, qkv_ref[:, channels:]).astype(bf16), keys, values)


def kept(rows, channels):
    pairs = channels // 128
    return [(pairs, 128, rows), (pairs, 2, rows, 128), (pairs, 144, rows)]


def project(own, qkv):
    rows, channels = own.shape
    return pl.pallas_call(
        project_kernel,
        out_shape=[jax.ShapeDtypeStruct(shape, bf16) for shape in kept(rows, channels)],
        in_specs=[vmem()] * 2,
        out_specs=[vmem()] * 3,
        compiler_params=params(20),
        cost_estimate=cost(6 * rows * channels * channels, 8 * rows * channels),
        name="project",
    )(own, qkv)


def space_kernel(
    queries, near_keys, near_values, peer_ref, stepped_ref, qkv_ref, out_ref, norm_ref,
    spaced_ref, normed_ref, keys, values, attended
):
    rows, channels = peer_ref.shape
    pairs = channels // 128
    keys[:, :, :rows] = near_keys[...]
    values[:, :, :rows] = near_values[...]
    split_heads(dot(peer_ref[...], qkv_ref[:, channels:]).astype(bf16), keys, values, rows)
    factor = 64 ** (-0.5) * LOG2E
    for j in range(pairs):
        q = queries[j]
        parts, weights = [], []
        for part in range(2):
            scores = dot(keys[j, part], q)
            top = jnp.max(scores, axis=0, keepdims=True)
            weights.append(jnp.exp2((scores - top) * factor).astype(bf16))
        for part in range(2):
            found = dot(values[j], weights[part])
            parts.append(found[part * 64 : part * 64 + 64] / found[128:129])
        attended[j] = jnp.concatenate(parts, axis=0).T.astype(bf16)
    joined = jnp.concatenate([attended[j] for j in range(pairs)], axis=1)
    spaced = stepped_ref[...] + dot(joined, out_ref[...])
    spaced_ref[...] = spaced
    normed_ref[...] = layer_norm(spaced, norm_ref[...])


def space(projected, peer, stepped, qkv, out, norm):
    rows, channels = peer.shape
    _, keys, values = kept(2 * rows, channels)
    return pl.pallas_call(
        space_kernel,
        out_shape=[
            jax.ShapeDtypeStruct((rows, channels), f32),
            jax.ShapeDtypeStruct((rows, channels), bf16),
        ],
        in_specs=[vmem()] * 8,
        out_specs=[vmem()] * 2,
        scratch_shapes=[
            pltpu.VMEM(keys, bf16),
            pltpu.VMEM(values, bf16),
            pltpu.VMEM((channels // 128, rows, 128), bf16),
        ],
        compiler_params=params(36),
        cost_estimate=cost(
            6 * rows * channels * channels + 8 * rows * rows * channels,
            14 * rows * channels,
            2 * HEADS * rows * rows,
        ),
        name="space",
    )(*projected, peer, stepped, qkv, out, norm)


def time_kernel_body(x_ref, qkv_ref, o_ref, packed_ref, turned, attended):
    frames, pixels, channels = x_ref.shape
    rows = frames * pixels
    pairs = channels // 128
    i = lax.broadcasted_iota(jnp.int32, (rows, rows), 0)
    j = lax.broadcasted_iota(jnp.int32, (rows, rows), 1)
    order = (j == (i % frames) * pixels + i // frames).astype(f32).astype(bf16)
    sorted_rows = dot(order, x_ref[...].reshape(rows, channels)).astype(bf16)
    packed = dot(sorted_rows, qkv_ref[...]).astype(bf16)
    packed_ref[...] = packed
    turned[...] = packed[:, channels : 2 * channels].T
    factor = 64 ** (-0.5) * LOG2E
    even, odd = half_masks((128, 128))
    above = lax.broadcasted_iota(jnp.int32, (128, 128), 0) < 64
    left = lax.broadcasted_iota(jnp.int32, (128, 128), 1) < 64
    same = above == left
    zero = jnp.zeros((128, 128), bf16)

    def two_pixels(at):
        for j in range(pairs):
            lanes = slice(j * 128, j * 128 + 128)
            q = packed_ref[at, lanes]
            v = packed_ref[at, 2 * channels + j * 128 : 2 * channels + j * 128 + 128]
            k = turned[lanes, at]
            keys = jnp.concatenate([jnp.where(above, k, zero), jnp.where(above, zero, k)], axis=1)
            scores = dot(q, keys)
            parts = []
            for part in range(2):
                own = jnp.where(same, scores[:, part * 128 : part * 128 + 128], -jnp.inf)
                top = jnp.max(own, axis=-1, keepdims=True)
                parts.append(jnp.exp2((own - top) * factor).astype(bf16))
            both = jnp.concatenate(
                [
                    jnp.concatenate([v * even, even], axis=1),
                    jnp.concatenate([v * odd, odd], axis=1),
                ],
                axis=0,
            )
            found = dot(jnp.concatenate(parts, axis=1), both)
            attended[at, lanes] = (found[:, :128] / found[:, 128:]).astype(bf16)

    for p in range(pixels // 2):
        two_pixels(slice(p * 128, p * 128 + 128))
    back = dot(order, attended[...], ((0,), (0,))).astype(bf16)
    o_ref[...] = back.reshape(frames, pixels, channels)


def time_attend(x, qkv):
    frames, pixels, channels = x.shape
    rows = frames * pixels
    return pl.pallas_call(
        time_kernel_body,
        out_shape=jax.ShapeDtypeStruct(x.shape, bf16),
        in_specs=[vmem()] * 2,
        out_specs=vmem(),
        scratch_shapes=[
            pltpu.VMEM((rows, 3 * channels), bf16),
            pltpu.VMEM((channels, rows), bf16),
            pltpu.VMEM((rows, channels), bf16),
        ],
        compiler_params=params(32),
        cost_estimate=cost(6 * rows * channels * channels + 4 * rows * rows * channels, 4 * rows * channels, HEADS * rows * frames),
        name="time_attend",
    )(x, qkv)


def finish_kernel(base_ref, x_ref, w_ref, o_ref):
    o_ref[...] = base_ref[...] + dot(x_ref[...], w_ref[...])


def finish(base, x, w):
    rows, channels = base.shape
    tile = rows // 2
    block = pl.BlockSpec((tile, channels), lambda i: (i, 0))
    return pl.pallas_call(
        finish_kernel,
        out_shape=jax.ShapeDtypeStruct((rows, channels), f32),
        grid=(rows // tile,),
        in_specs=[block, block, vmem()],
        out_specs=block,
        compiler_params=params(16),
        cost_estimate=cost(2 * rows * channels * channels, 10 * rows * channels),
        name="finish",
    )(base, x, w)


def body(
    latent, norm_gain, time_kernel, space_norm, space_qkv, space_out, time_norm, time_qkv, time_out
):
    frames, row_count, col_count, channels = latent.shape
    pixels = row_count * col_count
    assert frames == 1
    mine = latent.reshape(pixels, channels)
    count = lax.axis_size(FRAME)
    forward = [(i, i + 1) for i in range(count - 1)]
    backward = [(target, source) for source, target in forward]
    low = lax.ppermute(mine, FRAME, forward)
    high = lax.ppermute(mine, FRAME, backward)
    members = lax.axis_size(FRAME_ROW)
    sums = group_sums(mine, count)
    sums += lax.ppermute(sums, "row", [(0, 1), (1, 0)])
    sums = lax.all_to_all(sums, FRAME, split_axis=0, concat_axis=0, tiled=True)
    number = float(members * pixels * (channels // GROUPS))
    here = lax.axis_index(FRAME)
    edge = jnp.stack([here > 0, here < count - 1]).astype(jnp.int32)
    stepped, tokens = front(
        edge, sums, norm_gain.reshape(1, -1), low, mine, high, time_kernel,
        space_norm.reshape(1, -1), number,
    )
    peer = lax.ppermute(tokens, "row", [(0, 1), (1, 0)])
    projected = project(tokens, space_qkv)
    spaced, normed = space(projected, peer, stepped, space_qkv, space_out, time_norm.reshape(1, -1))
    moved = lax.all_to_all(
        normed.reshape(count, pixels // count, channels),
        FRAME, split_axis=0, concat_axis=0, tiled=True,
    )
    result = time_attend(moved, time_qkv)
    back = lax.all_to_all(result, FRAME, split_axis=0, concat_axis=0, tiled=True)
    output = finish(spaced, back.reshape(pixels, channels), time_out)
    return output.reshape(frames, row_count, col_count, channels)


def solution(mesh):
    split = P(("groups", "frame"), "row", None, None)
    return jax.shard_map(
        body,
        mesh=mesh,
        in_specs=(split,) + (P(),) * 8,
        out_specs=split,
        check_vma=False,
    )
```

```python
import functools

import jax
import jax.numpy as jnp
from jax import lax
from jax.experimental import pallas as pl
from jax.experimental.pallas import tpu as pltpu
from jax.sharding import PartitionSpec as P

HEADS = 10
GROUPS = 32
FRAME = "frame"
FRAME_ROW = ("frame", "row")
LOG2E = 1.4426950408889634

epsilon = 1e-05
f32 = jnp.float32
bf16 = jnp.bfloat16


def vmem():
    return pl.BlockSpec(memory_space=pltpu.VMEM)


def params(mib):
    return pltpu.CompilerParams(vmem_limit_bytes=mib << 20)


def cost(flops, nbytes, trans=0):
    return pl.CostEstimate(flops=flops, bytes_accessed=nbytes, transcendentals=trans)


def dot(a, b, dims=((1,), (0,)), precision=None):
    return lax.dot_general(
        a, b, (dims, ((), ())), preferred_element_type=f32, precision=precision
    )


def group_slots(channels):
    per_group = channels // GROUPS
    slot = lax.broadcasted_iota(jnp.int32, (128, channels), 0)
    chan = lax.broadcasted_iota(jnp.int32, (128, channels), 1)
    low = (slot % GROUPS) * per_group
    inside = (chan >= low) & (chan < low + per_group) & (slot < 2 * GROUPS)
    return jnp.where(inside, 1.0, 0.0).astype(bf16)


def pieces(x):
    high = x.astype(bf16).astype(f32)
    mid = (x - high).astype(bf16).astype(f32)
    return [high, mid, x - high - mid]


def stacked(first, second):
    rows = pieces(first) + pieces(second)
    return jnp.concatenate(rows + [jnp.zeros_like(first)] * 2, axis=0).astype(bf16)


def layer_norm(inputs, gain):
    center = jnp.mean(inputs, axis=-1, keepdims=True)
    shifted = inputs - center
    spread = jnp.mean(shifted * shifted, axis=-1, keepdims=True)
    return (shifted * lax.rsqrt(spread + epsilon) * gain).astype(bf16)


def sums_kernel(x_ref, o_ref, near, sem):
    rows, channels = x_ref.shape
    parts = 4
    tile = rows // parts
    copies = [
        pltpu.make_async_copy(
            x_ref.at[i * tile : i * tile + tile], near.at[i * tile : i * tile + tile], sem.at[i]
        )
        for i in range(parts)
    ]
    for copy in copies:
        copy.start()
    first = jnp.zeros((8, channels), f32)
    second = jnp.zeros((8, channels), f32)
    slots = group_slots(channels)
    for i, copy in enumerate(copies):
        copy.wait()
        x = near[i * tile : i * tile + tile].astype(f32).reshape(tile // 8, 8, channels)
        first += jnp.sum(x, axis=0)
        second += jnp.sum(x * x, axis=0)
    rows = stacked(jnp.sum(first, axis=0, keepdims=True), jnp.sum(second, axis=0, keepdims=True))
    total = dot(rows, slots, ((1,), (1,)))
    lane = lax.broadcasted_iota(jnp.int32, (1, 128), 1)
    row = jnp.where(
        lane < GROUPS,
        jnp.sum(total[0:3], axis=0, keepdims=True),
        jnp.sum(total[3:6], axis=0, keepdims=True),
    )
    o_ref[...] = jnp.broadcast_to(row[None], o_ref.shape)


def group_sums(latent, members):
    rows, channels = latent.shape
    return pl.pallas_call(
        sums_kernel,
        out_shape=jax.ShapeDtypeStruct((members, 1, 128), f32),
        in_specs=[pl.BlockSpec(memory_space=pltpu.HBM)],
        out_specs=vmem(),
        scratch_shapes=[pltpu.VMEM((rows, channels), bf16), pltpu.SemaphoreType.DMA((4,))],
        compiler_params=params(16),
        cost_estimate=cost(4 * rows * channels, 2 * rows * channels),
        name="group_sums",
    )(pin(latent))


def pin(x):
    return pltpu.with_memory_space_constraint(x, pltpu.HBM)


def front_kernel(
    number, edge_ref, sums_ref, gain_ref, low_ref, mid_ref, high_ref, kernel_far, norm_ref,
    stepped_ref, tokens_ref, scale, kernel_ref, sem
):
    channels = mid_ref.shape[1]
    first_step = pl.program_id(0) == 0
    get_kernel = pltpu.make_async_copy(kernel_far, kernel_ref, sem)

    @pl.when(first_step)
    def _():
        get_kernel.start()
        total = jnp.sum(sums_ref[...], axis=0)
        lane = lax.broadcasted_iota(jnp.int32, (1, 128), 1)
        none = jnp.zeros_like(total)
        rows = stacked(
            jnp.where(lane < GROUPS, total, none), jnp.where(lane < GROUPS, none, total)
        )
        spread = dot(rows, group_slots(channels))
        center = jnp.sum(spread[0:3], axis=0, keepdims=True) / number
        square = jnp.sum(spread[3:6], axis=0, keepdims=True) / number
        scaling = lax.rsqrt(square - center * center + epsilon) * gain_ref[...]
        scaling = jnp.broadcast_to(scaling, scale.shape[1:])
        center = jnp.broadcast_to(center, scale.shape[1:])
        scale[0] = scaling
        scale[1] = center
        get_kernel.wait()

    scaling, center = scale[0, 0:1], scale[1, 0:1]

    def hidden(ref):
        half = 0.5 * ((ref[...].astype(f32) - center) * scaling)
        return (half + half * jnp.tanh(half)).astype(bf16)

    low = hidden(low_ref)
    low = jnp.where(edge_ref[0] > 0, low, jnp.zeros_like(low))
    high = hidden(high_ref)
    high = jnp.where(edge_ref[1] > 0, high, jnp.zeros_like(high))
    mixed = dot(low, kernel_ref[0])
    mixed += dot(hidden(mid_ref), kernel_ref[1])
    mixed += dot(high, kernel_ref[2])
    stepped = mid_ref[...].astype(f32) + mixed
    stepped_ref[...] = stepped
    tokens_ref[...] = layer_norm(stepped, norm_ref[...])


def front(edge, sums, gain, low, mid, high, time_kernel, norm, number):
    rows, channels = mid.shape
    tile = rows // 2
    block = pl.BlockSpec((tile, channels), lambda i: (i, 0))
    one = pl.BlockSpec((1, channels), lambda i: (0, 0))
    return pl.pallas_call(
        functools.partial(front_kernel, number),
        out_shape=[
            jax.ShapeDtypeStruct((rows, channels), f32),
            jax.ShapeDtypeStruct((rows, channels), bf16),
        ],
        grid=(rows // tile,),
        in_specs=[
            pl.BlockSpec(memory_space=pltpu.SMEM),
            vmem(),
            one,
            block,
            block,
            block,
            pl.BlockSpec(memory_space=pltpu.HBM),
            one,
        ],
        out_specs=[block, block],
        scratch_shapes=[
            pltpu.VMEM((2, 8, channels), f32),
            pltpu.VMEM(time_kernel.shape, bf16),
            pltpu.SemaphoreType.DMA,
        ],
        compiler_params=params(24),
        cost_estimate=cost(6 * rows * channels * channels, 14 * rows * channels),
        name="front",
    )(edge, sums, gain, low, pin(mid), high, pin(time_kernel), norm)


def half_masks(shape):
    lane = lax.broadcasted_iota(jnp.int32, shape, len(shape) - 1)
    even = jnp.where(lane < 64, 1.0, 0.0).astype(bf16)
    odd = jnp.where(lane < 64, 0.0, 1.0).astype(bf16)
    return even, odd


def split_heads(packed, keys, values, at=0):
    rows, width = packed.shape
    channels = width // 2
    even, odd = half_masks((rows, 128))
    for j in range(channels // 128):
        k = packed[:, j * 128 : j * 128 + 128]
        v = packed[:, channels + j * 128 : channels + j * 128 + 128].T
        keys[j, 0, at : at + rows] = k * even
        keys[j, 1, at : at + rows] = k * odd
        values[j, :128, at : at + rows] = v
        values[j, 128:, at : at + rows] = jnp.ones((16, rows), bf16)


def project_kernel(own_ref, qkv_ref, queries, keys, values):
    channels = own_ref.shape[1]
    own = own_ref[...]
    factor = 64 ** (-0.5) * LOG2E
    packed = (dot(own, qkv_ref[:, :channels]) * factor).astype(bf16)
    for j in range(channels // 128):
        queries[j] = packed[:, j * 128 : j * 128 + 128].T
    split_heads(dot(own, qkv_ref[:, channels:]).astype(bf16), keys, values)


def kept(rows, channels):
    pairs = channels // 128
    return [(pairs, 128, rows), (pairs, 2, rows, 128), (pairs, 144, rows)]


def project(own, qkv):
    rows, channels = own.shape
    return pl.pallas_call(
        project_kernel,
        out_shape=[jax.ShapeDtypeStruct(shape, bf16) for shape in kept(rows, channels)],
        in_specs=[vmem()] * 2,
        out_specs=[vmem()] * 3,
        compiler_params=params(20),
        cost_estimate=cost(6 * rows * channels * channels, 8 * rows * channels),
        name="project",
    )(own, qkv)


def space_kernel(
    queries, near_keys, near_values, peer_ref, stepped_ref, qkv_ref, out_ref, norm_ref,
    spaced_ref, normed_ref, keys, values, attended
):
    rows, channels = peer_ref.shape
    pairs = channels // 128
    keys[:, :, :rows] = near_keys[...]
    values[:, :, :rows] = near_values[...]
    split_heads(dot(peer_ref[...], qkv_ref[:, channels:]).astype(bf16), keys, values, rows)
    for j in range(pairs):
        q = queries[j]
        parts, weights = [], []
        for part in range(2):
            scores = dot(keys[j, part], q)
            top = jnp.max(scores, axis=0, keepdims=True)
            weights.append(jnp.exp2(scores - top).astype(bf16))
        for part in range(2):
            found = dot(values[j], weights[part])
            parts.append(found[part * 64 : part * 64 + 64] / found[128:129])
        attended[j] = jnp.concatenate(parts, axis=0).T.astype(bf16)
    joined = jnp.concatenate([attended[j] for j in range(pairs)], axis=1)
    spaced = stepped_ref[...] + dot(joined, out_ref[...])
    spaced_ref[...] = spaced
    normed_ref[...] = layer_norm(spaced, norm_ref[...])


def space(projected, peer, stepped, qkv, out, norm):
    rows, channels = peer.shape
    _, keys, values = kept(2 * rows, channels)
    return pl.pallas_call(
        space_kernel,
        out_shape=[
            jax.ShapeDtypeStruct((rows, channels), f32),
            jax.ShapeDtypeStruct((rows, channels), bf16),
        ],
        in_specs=[vmem()] * 8,
        out_specs=[vmem()] * 2,
        scratch_shapes=[
            pltpu.VMEM(keys, bf16),
            pltpu.VMEM(values, bf16),
            pltpu.VMEM((channels // 128, rows, 128), bf16),
        ],
        compiler_params=params(36),
        cost_estimate=cost(
            6 * rows * channels * channels + 8 * rows * rows * channels,
            14 * rows * channels,
            2 * HEADS * rows * rows,
        ),
        name="space",
    )(*projected, peer, stepped, qkv, out, norm)


def time_kernel_body(x_ref, qkv_ref, o_ref, packed_ref, turned, attended):
    frames, pixels, channels = x_ref.shape
    rows = frames * pixels
    pairs = channels // 128
    i = lax.broadcasted_iota(jnp.int32, (rows, rows), 0)
    j = lax.broadcasted_iota(jnp.int32, (rows, rows), 1)
    order = (j == (i % frames) * pixels + i // frames).astype(f32).astype(bf16)
    sorted_rows = dot(order, x_ref[...].reshape(rows, channels)).astype(bf16)
    packed = dot(sorted_rows, qkv_ref[...]).astype(bf16)
    packed_ref[...] = packed
    turned[...] = packed[:, channels : 2 * channels].T
    factor = 64 ** (-0.5) * LOG2E
    even, odd = half_masks((128, 128))
    above = lax.broadcasted_iota(jnp.int32, (128, 128), 0) < 64
    left = lax.broadcasted_iota(jnp.int32, (128, 128), 1) < 64
    same = above == left
    zero = jnp.zeros((128, 128), bf16)

    def two_pixels(at):
        for j in range(pairs):
            lanes = slice(j * 128, j * 128 + 128)
            q = packed_ref[at, lanes]
            v = packed_ref[at, 2 * channels + j * 128 : 2 * channels + j * 128 + 128]
            k = turned[lanes, at]
            keys = jnp.concatenate([jnp.where(above, k, zero), jnp.where(above, zero, k)], axis=1)
            scores = dot(q, keys)
            parts = []
            for part in range(2):
                own = jnp.where(same, scores[:, part * 128 : part * 128 + 128], -jnp.inf)
                top = jnp.max(own, axis=-1, keepdims=True)
                parts.append(jnp.exp2((own - top) * factor).astype(bf16))
            both = jnp.concatenate(
                [
                    jnp.concatenate([v * even, even], axis=1),
                    jnp.concatenate([v * odd, odd], axis=1),
                ],
                axis=0,
            )
            found = dot(jnp.concatenate(parts, axis=1), both)
            attended[at, lanes] = (found[:, :128] / found[:, 128:]).astype(bf16)

    for p in range(pixels // 2):
        two_pixels(slice(p * 128, p * 128 + 128))
    back = dot(order, attended[...], ((0,), (0,))).astype(bf16)
    o_ref[...] = back.reshape(frames, pixels, channels)


def time_attend(x, qkv):
    frames, pixels, channels = x.shape
    rows = frames * pixels
    return pl.pallas_call(
        time_kernel_body,
        out_shape=jax.ShapeDtypeStruct(x.shape, bf16),
        in_specs=[vmem()] * 2,
        out_specs=vmem(),
        scratch_shapes=[
            pltpu.VMEM((rows, 3 * channels), bf16),
            pltpu.VMEM((channels, rows), bf16),
            pltpu.VMEM((rows, channels), bf16),
        ],
        compiler_params=params(32),
        cost_estimate=cost(6 * rows * channels * channels + 4 * rows * rows * channels, 4 * rows * channels, HEADS * rows * frames),
        name="time_attend",
    )(x, qkv)


def finish_kernel(base_ref, x_ref, w_ref, o_ref):
    o_ref[...] = base_ref[...] + dot(x_ref[...], w_ref[...])


def finish(base, x, w):
    rows, channels = base.shape
    tile = rows // 2
    block = pl.BlockSpec((tile, channels), lambda i: (i, 0))
    return pl.pallas_call(
        finish_kernel,
        out_shape=jax.ShapeDtypeStruct((rows, channels), f32),
        grid=(rows // tile,),
        in_specs=[block, block, vmem()],
        out_specs=block,
        compiler_params=params(16),
        cost_estimate=cost(2 * rows * channels * channels, 10 * rows * channels),
        name="finish",
    )(base, x, w)


def body(
    latent, norm_gain, time_kernel, space_norm, space_qkv, space_out, time_norm, time_qkv, time_out
):
    frames, row_count, col_count, channels = latent.shape
    pixels = row_count * col_count
    assert frames == 1
    mine = latent.reshape(pixels, channels)
    count = lax.axis_size(FRAME)
    forward = [(i, i + 1) for i in range(count - 1)]
    backward = [(target, source) for source, target in forward]
    low = lax.ppermute(mine, FRAME, forward)
    high = lax.ppermute(mine, FRAME, backward)
    members = lax.axis_size(FRAME_ROW)
    sums = group_sums(mine, count)
    sums += lax.ppermute(sums, "row", [(0, 1), (1, 0)])
    sums = lax.all_to_all(sums, FRAME, split_axis=0, concat_axis=0, tiled=True)
    number = float(members * pixels * (channels // GROUPS))
    here = lax.axis_index(FRAME)
    edge = jnp.stack([here > 0, here < count - 1]).astype(jnp.int32)
    stepped, tokens = front(
        edge, sums, norm_gain.reshape(1, -1), low, mine, high, time_kernel,
        space_norm.reshape(1, -1), number,
    )
    peer = lax.ppermute(tokens, "row", [(0, 1), (1, 0)])
    projected = project(tokens, space_qkv)
    spaced, normed = space(projected, peer, stepped, space_qkv, space_out, time_norm.reshape(1, -1))
    moved = lax.all_to_all(
        normed.reshape(count, pixels // count, channels),
        FRAME, split_axis=0, concat_axis=0, tiled=True,
    )
    result = time_attend(moved, time_qkv)
    back = lax.all_to_all(result, FRAME, split_axis=0, concat_axis=0, tiled=True)
    output = finish(spaced, back.reshape(pixels, channels), time_out)
    return output.reshape(frames, row_count, col_count, channels)


def solution(mesh):
    split = P(("groups", "frame"), "row", None, None)
    return jax.shard_map(
        body,
        mesh=mesh,
        in_specs=(split,) + (P(),) * 8,
        out_specs=split,
        check_vma=False,
    )
```

```python
import functools

import jax
import jax.numpy as jnp
from jax import lax
from jax.experimental import pallas as pl
from jax.experimental.pallas import tpu as pltpu
from jax.sharding import PartitionSpec as P

HEADS = 10
GROUPS = 32
FRAME = "frame"
FRAME_ROW = ("frame", "row")
LOG2E = 1.4426950408889634

epsilon = 1e-05
f32 = jnp.float32
bf16 = jnp.bfloat16


def vmem():
    return pl.BlockSpec(memory_space=pltpu.VMEM)


def params(mib):
    return pltpu.CompilerParams(vmem_limit_bytes=mib << 20)


def cost(flops, nbytes, trans=0):
    return pl.CostEstimate(flops=flops, bytes_accessed=nbytes, transcendentals=trans)


def dot(a, b, dims=((1,), (0,)), precision=None):
    return lax.dot_general(
        a, b, (dims, ((), ())), preferred_element_type=f32, precision=precision
    )


def group_slots(channels):
    per_group = channels // GROUPS
    slot = lax.broadcasted_iota(jnp.int32, (128, channels), 0)
    chan = lax.broadcasted_iota(jnp.int32, (128, channels), 1)
    low = (slot % GROUPS) * per_group
    inside = (chan >= low) & (chan < low + per_group) & (slot < 2 * GROUPS)
    return jnp.where(inside, 1.0, 0.0).astype(bf16)


def pieces(x):
    high = x.astype(bf16).astype(f32)
    mid = (x - high).astype(bf16).astype(f32)
    return [high, mid, x - high - mid]


def stacked(first, second):
    rows = pieces(first) + pieces(second)
    return jnp.concatenate(rows + [jnp.zeros_like(first)] * 2, axis=0).astype(bf16)


def layer_norm(inputs, gain):
    center = jnp.mean(inputs, axis=-1, keepdims=True)
    shifted = inputs - center
    spread = jnp.mean(shifted * shifted, axis=-1, keepdims=True)
    return (shifted * lax.rsqrt(spread + epsilon) * gain).astype(bf16)


def sums_kernel(x_ref, o_ref, near, sem):
    rows, channels = x_ref.shape
    parts = 4
    tile = rows // parts
    copies = [
        pltpu.make_async_copy(
            x_ref.at[i * tile : i * tile + tile], near.at[i * tile : i * tile + tile], sem.at[i]
        )
        for i in range(parts)
    ]
    for copy in copies:
        copy.start()
    first = jnp.zeros((8, channels), f32)
    second = jnp.zeros((8, channels), f32)
    slots = group_slots(channels)
    for i, copy in enumerate(copies):
        copy.wait()
        x = near[i * tile : i * tile + tile].astype(f32).reshape(tile // 8, 8, channels)
        first += jnp.sum(x, axis=0)
        second += jnp.sum(x * x, axis=0)
    rows = stacked(jnp.sum(first, axis=0, keepdims=True), jnp.sum(second, axis=0, keepdims=True))
    total = dot(rows, slots, ((1,), (1,)))
    lane = lax.broadcasted_iota(jnp.int32, (1, 128), 1)
    row = jnp.where(
        lane < GROUPS,
        jnp.sum(total[0:3], axis=0, keepdims=True),
        jnp.sum(total[3:6], axis=0, keepdims=True),
    )
    o_ref[...] = jnp.broadcast_to(row[None], o_ref.shape)


def group_sums(latent, members):
    rows, channels = latent.shape
    return pl.pallas_call(
        sums_kernel,
        out_shape=jax.ShapeDtypeStruct((members, 1, 128), f32),
        in_specs=[pl.BlockSpec(memory_space=pltpu.HBM)],
        out_specs=vmem(),
        scratch_shapes=[pltpu.VMEM((rows, channels), bf16), pltpu.SemaphoreType.DMA((4,))],
        compiler_params=params(16),
        cost_estimate=cost(4 * rows * channels, 2 * rows * channels),
        name="group_sums",
    )(pin(latent))


def pin(x):
    return pltpu.with_memory_space_constraint(x, pltpu.HBM)


def front_kernel(
    number, edge_ref, sums_ref, others_ref, gain_ref, low_ref, mid_ref, high_ref, kernel_far, norm_ref,
    stepped_ref, tokens_ref, scale, kernel_ref, sem
):
    channels = mid_ref.shape[1]
    first_step = pl.program_id(0) == 0
    get_kernel = pltpu.make_async_copy(kernel_far, kernel_ref, sem)

    @pl.when(first_step)
    def _():
        get_kernel.start()
        total = jnp.sum(sums_ref[...] + others_ref[...], axis=0)
        lane = lax.broadcasted_iota(jnp.int32, (1, 128), 1)
        none = jnp.zeros_like(total)
        rows = stacked(
            jnp.where(lane < GROUPS, total, none), jnp.where(lane < GROUPS, none, total)
        )
        spread = dot(rows, group_slots(channels))
        center = jnp.sum(spread[0:3], axis=0, keepdims=True) / number
        square = jnp.sum(spread[3:6], axis=0, keepdims=True) / number
        scaling = lax.rsqrt(square - center * center + epsilon) * gain_ref[...]
        scaling = jnp.broadcast_to(scaling, scale.shape[1:])
        center = jnp.broadcast_to(center, scale.shape[1:])
        scale[0] = scaling
        scale[1] = center
        get_kernel.wait()

    scaling, center = scale[0, 0:1], scale[1, 0:1]

    def hidden(ref):
        half = 0.5 * ((ref[...].astype(f32) - center) * scaling)
        return (half + half * jnp.tanh(half)).astype(bf16)

    low = hidden(low_ref)
    low = jnp.where(edge_ref[0] > 0, low, jnp.zeros_like(low))
    high = hidden(high_ref)
    high = jnp.where(edge_ref[1] > 0, high, jnp.zeros_like(high))
    mixed = dot(low, kernel_ref[0])
    mixed += dot(hidden(mid_ref), kernel_ref[1])
    mixed += dot(high, kernel_ref[2])
    stepped = mid_ref[...].astype(f32) + mixed
    stepped_ref[...] = stepped
    tokens_ref[...] = layer_norm(stepped, norm_ref[...])


def front(edge, sums, others, gain, low, mid, high, time_kernel, norm, number):
    rows, channels = mid.shape
    tile = rows // 2
    block = pl.BlockSpec((tile, channels), lambda i: (i, 0))
    one = pl.BlockSpec((1, channels), lambda i: (0, 0))
    return pl.pallas_call(
        functools.partial(front_kernel, number),
        out_shape=[
            jax.ShapeDtypeStruct((rows, channels), f32),
            jax.ShapeDtypeStruct((rows, channels), bf16),
        ],
        grid=(rows // tile,),
        in_specs=[
            pl.BlockSpec(memory_space=pltpu.SMEM),
            vmem(),
            vmem(),
            one,
            block,
            block,
            block,
            pl.BlockSpec(memory_space=pltpu.HBM),
            one,
        ],
        out_specs=[block, block],
        scratch_shapes=[
            pltpu.VMEM((2, 8, channels), f32),
            pltpu.VMEM(time_kernel.shape, bf16),
            pltpu.SemaphoreType.DMA,
        ],
        compiler_params=params(24),
        cost_estimate=cost(6 * rows * channels * channels, 14 * rows * channels),
        name="front",
    )(edge, sums, others, gain, low, pin(mid), high, pin(time_kernel), norm)


def half_masks(shape):
    lane = lax.broadcasted_iota(jnp.int32, shape, len(shape) - 1)
    even = jnp.where(lane < 64, 1.0, 0.0).astype(bf16)
    odd = jnp.where(lane < 64, 0.0, 1.0).astype(bf16)
    return even, odd


def split_heads(packed, keys, values, at=0):
    rows, width = packed.shape
    channels = width // 2
    even, odd = half_masks((rows, 128))
    for j in range(channels // 128):
        k = packed[:, j * 128 : j * 128 + 128]
        v = packed[:, channels + j * 128 : channels + j * 128 + 128].T
        keys[j, 0, at : at + rows] = k * even
        keys[j, 1, at : at + rows] = k * odd
        values[j, :128, at : at + rows] = v
        values[j, 128:, at : at + rows] = jnp.ones((16, rows), bf16)


def project_kernel(own_ref, qkv_ref, queries, keys, values):
    channels = own_ref.shape[1]
    own = own_ref[...]
    factor = 64 ** (-0.5) * LOG2E
    packed = (dot(own, qkv_ref[:, :channels]) * factor).astype(bf16)
    for j in range(channels // 128):
        queries[j] = packed[:, j * 128 : j * 128 + 128].T
    split_heads(dot(own, qkv_ref[:, channels:]).astype(bf16), keys, values)


def kept(rows, channels):
    pairs = channels // 128
    return [(pairs, 128, rows), (pairs, 2, rows, 128), (pairs, 144, rows)]


def project(own, qkv):
    rows, channels = own.shape
    return pl.pallas_call(
        project_kernel,
        out_shape=[jax.ShapeDtypeStruct(shape, bf16) for shape in kept(rows, channels)],
        in_specs=[vmem()] * 2,
        out_specs=[vmem()] * 3,
        compiler_params=params(20),
        cost_estimate=cost(6 * rows * channels * channels, 8 * rows * channels),
        name="project",
    )(own, qkv)


def space_kernel(
    queries, near_keys, near_values, peer_ref, stepped_ref, qkv_ref, out_ref, norm_ref,
    spaced_ref, normed_ref, keys, values, attended
):
    rows, channels = peer_ref.shape
    pairs = channels // 128
    keys[:, :, :rows] = near_keys[...]
    values[:, :, :rows] = near_values[...]
    split_heads(dot(peer_ref[...], qkv_ref[:, channels:]).astype(bf16), keys, values, rows)
    for j in range(pairs):
        q = queries[j]
        parts, weights = [], []
        for part in range(2):
            scores = dot(keys[j, part], q)
            top = jnp.max(scores, axis=0, keepdims=True)
            weights.append(jnp.exp2(scores - top).astype(bf16))
        for part in range(2):
            found = dot(values[j], weights[part])
            parts.append(found[part * 64 : part * 64 + 64] / found[128:129])
        attended[j] = jnp.concatenate(parts, axis=0).T.astype(bf16)
    joined = jnp.concatenate([attended[j] for j in range(pairs)], axis=1)
    spaced = stepped_ref[...] + dot(joined, out_ref[...])
    spaced_ref[...] = spaced
    normed_ref[...] = layer_norm(spaced, norm_ref[...])


def space(projected, peer, stepped, qkv, out, norm):
    rows, channels = peer.shape
    _, keys, values = kept(2 * rows, channels)
    return pl.pallas_call(
        space_kernel,
        out_shape=[
            jax.ShapeDtypeStruct((rows, channels), f32),
            jax.ShapeDtypeStruct((rows, channels), bf16),
        ],
        in_specs=[vmem()] * 8,
        out_specs=[vmem()] * 2,
        scratch_shapes=[
            pltpu.VMEM(keys, bf16),
            pltpu.VMEM(values, bf16),
            pltpu.VMEM((channels // 128, rows, 128), bf16),
        ],
        compiler_params=params(36),
        cost_estimate=cost(
            6 * rows * channels * channels + 8 * rows * rows * channels,
            14 * rows * channels,
            2 * HEADS * rows * rows,
        ),
        name="space",
    )(*projected, peer, stepped, qkv, out, norm)


def time_kernel_body(x_ref, qkv_ref, o_ref, packed_ref, turned, attended):
    frames, pixels, channels = x_ref.shape
    rows = frames * pixels
    pairs = channels // 128
    i = lax.broadcasted_iota(jnp.int32, (rows, rows), 0)
    j = lax.broadcasted_iota(jnp.int32, (rows, rows), 1)
    order = (j == (i % frames) * pixels + i // frames).astype(f32).astype(bf16)
    sorted_rows = dot(order, x_ref[...].reshape(rows, channels)).astype(bf16)
    packed = dot(sorted_rows, qkv_ref[...]).astype(bf16)
    packed_ref[...] = packed
    turned[...] = packed[:, channels : 2 * channels].T
    factor = 64 ** (-0.5) * LOG2E
    even, odd = half_masks((128, 128))
    above = lax.broadcasted_iota(jnp.int32, (128, 128), 0) < 64
    left = lax.broadcasted_iota(jnp.int32, (128, 128), 1) < 64
    same = above == left
    zero = jnp.zeros((128, 128), bf16)

    def two_pixels(at):
        for j in range(pairs):
            lanes = slice(j * 128, j * 128 + 128)
            q = packed_ref[at, lanes]
            v = packed_ref[at, 2 * channels + j * 128 : 2 * channels + j * 128 + 128]
            k = turned[lanes, at]
            keys = jnp.concatenate([jnp.where(above, k, zero), jnp.where(above, zero, k)], axis=1)
            scores = dot(q, keys)
            parts = []
            for part in range(2):
                own = jnp.where(same, scores[:, part * 128 : part * 128 + 128], -jnp.inf)
                top = jnp.max(own, axis=-1, keepdims=True)
                parts.append(jnp.exp2((own - top) * factor).astype(bf16))
            both = jnp.concatenate(
                [
                    jnp.concatenate([v * even, even], axis=1),
                    jnp.concatenate([v * odd, odd], axis=1),
                ],
                axis=0,
            )
            found = dot(jnp.concatenate(parts, axis=1), both)
            attended[at, lanes] = (found[:, :128] / found[:, 128:]).astype(bf16)

    for p in range(pixels // 2):
        two_pixels(slice(p * 128, p * 128 + 128))
    back = dot(order, attended[...], ((0,), (0,))).astype(bf16)
    o_ref[...] = back.reshape(frames, pixels, channels)


def time_attend(x, qkv):
    frames, pixels, channels = x.shape
    rows = frames * pixels
    return pl.pallas_call(
        time_kernel_body,
        out_shape=jax.ShapeDtypeStruct(x.shape, bf16),
        in_specs=[vmem()] * 2,
        out_specs=vmem(),
        scratch_shapes=[
            pltpu.VMEM((rows, 3 * channels), bf16),
            pltpu.VMEM((channels, rows), bf16),
            pltpu.VMEM((rows, channels), bf16),
        ],
        compiler_params=params(32),
        cost_estimate=cost(6 * rows * channels * channels + 4 * rows * rows * channels, 4 * rows * channels, HEADS * rows * frames),
        name="time_attend",
    )(x, qkv)


def finish_kernel(base_ref, x_ref, w_ref, o_ref):
    o_ref[...] = base_ref[...] + dot(x_ref[...], w_ref[...])


def finish(base, x, w):
    rows, channels = base.shape
    tile = rows // 2
    block = pl.BlockSpec((tile, channels), lambda i: (i, 0))
    return pl.pallas_call(
        finish_kernel,
        out_shape=jax.ShapeDtypeStruct((rows, channels), f32),
        grid=(rows // tile,),
        in_specs=[block, block, vmem()],
        out_specs=block,
        compiler_params=params(16),
        cost_estimate=cost(2 * rows * channels * channels, 10 * rows * channels),
        name="finish",
    )(base, x, w)


def body(
    latent, norm_gain, time_kernel, space_norm, space_qkv, space_out, time_norm, time_qkv, time_out
):
    frames, row_count, col_count, channels = latent.shape
    pixels = row_count * col_count
    assert frames == 1
    mine = latent.reshape(pixels, channels)
    count = lax.axis_size(FRAME)
    forward = [(i, i + 1) for i in range(count - 1)]
    backward = [(target, source) for source, target in forward]
    low = lax.ppermute(mine, FRAME, forward)
    high = lax.ppermute(mine, FRAME, backward)
    members = lax.axis_size(FRAME_ROW)
    sums = group_sums(mine, count)
    sums = lax.all_to_all(sums, FRAME, split_axis=0, concat_axis=0, tiled=True)
    others = lax.ppermute(sums, "row", [(0, 1), (1, 0)])
    number = float(members * pixels * (channels // GROUPS))
    here = lax.axis_index(FRAME)
    edge = jnp.stack([here > 0, here < count - 1]).astype(jnp.int32)
    stepped, tokens = front(
        edge, sums, others, norm_gain.reshape(1, -1), low, mine, high, time_kernel,
        space_norm.reshape(1, -1), number,
    )
    peer = lax.ppermute(tokens, "row", [(0, 1), (1, 0)])
    projected = project(tokens, space_qkv)
    spaced, normed = space(projected, peer, stepped, space_qkv, space_out, time_norm.reshape(1, -1))
    moved = lax.all_to_all(
        normed.reshape(count, pixels // count, channels),
        FRAME, split_axis=0, concat_axis=0, tiled=True,
    )
    result = time_attend(moved, time_qkv)
    back = lax.all_to_all(result, FRAME, split_axis=0, concat_axis=0, tiled=True)
    output = finish(spaced, back.reshape(pixels, channels), time_out)
    return output.reshape(frames, row_count, col_count, channels)


def solution(mesh):
    split = P(("groups", "frame"), "row", None, None)
    return jax.shard_map(
        body,
        mesh=mesh,
        in_specs=(split,) + (P(),) * 8,
        out_specs=split,
        check_vma=False,
    )
```
